512 devices in a mesh: hot: 32 (over y, x, core), tt: 16 (over z).
Axes of the slice: x: 4, y: 4, z: 16, core: 2. Of those that a mesh axis runs over, the one named last changes fastest.
Arguments:
- hot_table: float32 [8192, 256], P('hot'), may hold values from -1.5 to 1.5
- hot_accum: float32 [8192], P('hot'), may hold values from 0.05 to 1
- hot_owner: int32 [131072, 1], P(('hot', 'tt')), may hold values from 0 to 31; in each aligned block of 256 rows (0 to 255, 256 to 511, ...) at most 16 rows name the same one
- hot_row: int32 [512, 256], P(('hot', 'tt')), may hold values from 0 to 255
- hot_bag: int32 [512, 256], P(('hot', 'tt')), may hold values from 0 to 63, never falling along the last dimension, each value on 1 to 12 neighbouring positions
- cold_owner: int32 [262144, 1], P(('hot', 'tt')), may hold values from 0 to 15; in each aligned block of 512 rows (0 to 511, 512 to 1023, ...) at most 64 rows name the same one
- first_index: int32 [512, 512], P(('hot', 'tt')), may hold values from 0 to 127
- mid_index: int32 [512, 512], P(('hot', 'tt')), may hold values from 0 to 63
- last_index: int32 [512, 512], P(('hot', 'tt')), may hold values from 0 to 63
- cold_bag: int32 [512, 512], P(('hot', 'tt')), may hold values from 0 to 63, never falling along the last dimension, each value on 1 to 24 neighbouring positions
- core_first: float32 [2048, 256], P('tt'), may hold values from -1 to 1
- core_mid: bfloat16 [64, 8192], replicated, may hold values from -1 to 1
- core_last: bfloat16 [64, 128], replicated, may hold values from -6 to 6
- bag_grads: bfloat16 [32768, 256], P(('hot', 'tt')), may hold values from -6 to 6
Outputs:
- pooled: float32 [32768, 256], P(('hot', 'tt'))
- new_table: float32 [8192, 256], P('hot')
- new_accum: float32 [8192], P('hot')
- new_first: float32 [2048, 256], P('tt')
The draws below stay inside these ranges and needn't reach their ends.
Inputs may be any that keep to these rules, and one draw needn't show every extreme that they name: `hot_owner`: among the 256 hot lookups of one device no owner appears more than 16 times; some owner appears exactly that often. `cold_owner`: among the 512 cold lookups of one device no owner appears more than 64 times; some owner appears exactly that often. `hot_bag`: never falling along a device's lookups; every bag of a device has at least one hot lookup. `cold_bag`: never falling along a device's lookups; every bag of a device has at least one cold lookup.
All inputs are finite; a program needn't handle non-finite values.
Results may differ from the reference program's by a relative error of at most 0.005.
Values may be sent and summed in bfloat16 or wider, within the bound.
A program may use at most 64 MiB of HBM per device.

```python
import math
import jax
import jax.numpy as jnp
import numpy as np
from jax import lax

E1 = 8
E2 = 8
E3 = 4
RANK = 32
HOT_DEV = 256
HOT_LOOK = 256
COLD_LOOK = 512
BAGS_DEV = 64
SLICE_DEV = 128
MID_SLICES = 64
LAST_SLICES = 64
E = 256
CAP_HOT = 16
CAP_COLD = 64
N_HOT = 32
N_TT = 16
DEVICES = 512


def touch_ends(values, key, least, top_value):
    place = [jax.random.randint(jax.random.fold_in(key, axis), (), 0, length) for axis, length in enumerate(values.shape)]
    main_axis = values.shape.index(max(values.shape))
    beside = place[:main_axis] + [(place[main_axis] + 1) % values.shape[main_axis]] + place[main_axis + 1:]
    return values.at[tuple(place)].set(least).at[tuple(beside)].set(top_value)


def levels(key, extent, cuts, low, high):
    def one(axis_at, shards_of):
        draws = jax.random.uniform(jax.random.fold_in(jax.random.fold_in(key, 6), axis_at), (shards_of,), jnp.float32, low / len(cuts), high / len(cuts))
        return jnp.repeat(jnp.exp(draws), extent[axis_at] // shards_of).reshape((-1,) + (1,) * (len(extent) - axis_at - 1))

    level = one(*cuts[0])
    for cut in cuts[1:]:
        level = level * one(*cut)
    return level


def rank_bounds(count, slope):
    portions = [(1 << 20) // math.isqrt(rank ** slope) + 1 for rank in range(1, count + 1)]
    deviation = 1 + sum(portions) // (1 << 30)
    return np.cumsum(np.array([max(1, weight // deviation) for weight in portions]))


def ranked_ids(stream_key, shape, amount, skew):
    grid = rank_bounds(amount, skew)
    pick = jax.random.randint(jax.random.fold_in(stream_key, 1), shape, 0, int(grid[amount - 1]))
    grade = jnp.searchsorted(jnp.asarray(grid, jnp.int32), pick, side="right")
    return jax.random.permutation(jax.random.fold_in(stream_key, 2), amount)[grade].astype(jnp.int32)


def split_up(count, total, limit, lean):
    portions = [(1 << 20) // math.isqrt(rank ** lean) + 1 for rank in range(2, count + 1)]
    surplus, given = total - limit - (count - 1), [1] * (count - 1)
    while surplus > 0:
        candidates = [i for i in range(count - 1) if given[i] < limit]
        whole, left = sum([portions[i] for i in candidates]), surplus
        for i in candidates:
            more = min(limit - given[i], max(1, left * portions[i] // whole), surplus)
            given[i] = given[i] + more
            surplus = surplus - more
    return np.array([limit] + given)


def ragged_sizes(rng, number_of, total, bound, slope):
    if number_of == 2:
        one = jax.random.randint(rng, (), max(1, total - bound), min(bound, total - 1) + 1)
        return jnp.stack([one, total - one])
    sizes = jnp.asarray(split_up(number_of, total, bound, slope), jnp.int32)
    twos = (number_of - 1) // 2
    source_of, taker = sizes[1:1 + 2 * twos:2], sizes[2:2 + 2 * twos:2]
    slack = jnp.minimum(source_of - 1, bound - taker)
    shifted = jax.random.randint(jax.random.fold_in(rng, 1), (twos,), 0, 1 << 20) % (slack + 1)
    sizes = sizes.at[1:1 + 2 * twos:2].set(source_of - shifted).at[2:2 + 2 * twos:2].set(taker + shifted)
    return sizes[jax.random.permutation(jax.random.fold_in(rng, 2), number_of)]


def deal_out(own_key, own, number, rows, number_of, top, most, lean):
    sequence = jax.random.permutation(own_key, number_of)
    heavy_load, common = portions_of(number_of, rows * top, most, lean, True), portions_of(number_of, rows * top, most, lean, False)
    places = jnp.arange(number_of)

    def named(tallies, rotation):
        used = int((tallies > 0).sum())
        fixed = max(1, used // 4)
        moved = fixed + (places - fixed + rotation * (used - fixed)) % max(1, number_of - fixed)
        return jnp.zeros((number_of,), jnp.int32).at[sequence[jnp.where(places < fixed, places, moved)]].set(jnp.asarray(tallies, jnp.int32))

    tallies = jnp.where(number % 4 == 0, named(heavy_load, number // 4), named(common, number - number // 4 - 1))
    mixed = jax.random.permutation(jax.random.fold_in(own, 3), number_of)
    giver, receiver = mixed[0:number_of // 2 * 2:2], mixed[1:number_of // 2 * 2:2]
    room = jnp.minimum(tallies[giver] - 1, most - tallies[receiver]) // 2
    room = jnp.where((giver == sequence[0]) | (receiver == sequence[0]) | (tallies[receiver] == 0), 0, jnp.maximum(room, 0))
    moved = jax.random.randint(jax.random.fold_in(own, 4), (number_of // 2,), 0, 1 << 20) % (room + 1)
    tallies = tallies.at[giver].add(-moved).at[receiver].add(moved)
    members = jnp.searchsorted(jnp.cumsum(tallies), jnp.arange(rows * top), side="right").astype(jnp.int32)
    table = members.reshape(top, rows).T
    table = table[jax.random.permutation(jax.random.fold_in(own, 1), rows)]
    rotation = jax.random.randint(jax.random.fold_in(own, 2), (rows, 1), 0, top)
    return jnp.take_along_axis(table, (jnp.arange(top)[None, :] + rotation) % top, axis=1)


def portions_of(number_of, total, bound, lean, full):
    loads = [(1 << 20) // math.isqrt(rank ** lean) + 1 for rank in range(1, number_of + 1)]
    largest = bound if full else min(bound, max(-(-total // number_of), total * loads[0] // sum(loads)))
    least = 1 if total - largest >= number_of - 1 else 0
    holding, rest = [largest] + [least] * (number_of - 1), total - largest - least * (number_of - 1)
    while rest > 0:
        candidates = [i for i in range(1, number_of) if holding[i] < largest] or [i for i in range(1, number_of) if holding[i] < bound]
        pool, left = sum([loads[i] for i in candidates]), rest
        for i in candidates:
            addition = min(bound - holding[i], max(1, left * loads[i] // pool), rest)
            holding[i] = holding[i] + addition
            rest = rest - addition
    return np.array(holding)


def scatter_about(rng, extent, deviation, reach, shards=(), held_as=jnp.bfloat16):
    entries = jax.random.normal(rng, extent, jnp.float32) * deviation
    if len(shards) > 0:
        entries = levels(rng, extent, shards, -0.22, 0.18) * entries
    return jnp.clip(entries, min=-reach, max=reach).astype(held_as)


def setup_inputs(seed: int = 0) -> dict:
    arg_keys = jax.random.split(jax.random.key(seed), 15)
    hot_table = scatter_about(arg_keys[0], (N_HOT * HOT_DEV, E), 0.25, 1.5, ((0, 32),), jnp.float32)
    hot_accum = jnp.clip(jnp.exp(math.log(1.0) - 2.9957323 * jax.random.uniform(arg_keys[1], (N_HOT * HOT_DEV,), jnp.float32) ** levels(arg_keys[1], (N_HOT * HOT_DEV,), ((0, 32),), -0.2, 0.2)), 0.05, 1.0)
    hot_owner_keys = jax.random.split(jax.random.fold_in(arg_keys[2], 1), (DEVICES * HOT_LOOK) // HOT_LOOK)
    hot_owner_turns = jax.random.permutation(jax.random.fold_in(arg_keys[2], 3), (DEVICES * HOT_LOOK) // HOT_LOOK)
    hot_owner = jax.vmap(lambda own, number: deal_out(jax.random.fold_in(arg_keys[2], 2), own, number, HOT_LOOK, N_HOT, 1, CAP_HOT, 2))(hot_owner_keys, hot_owner_turns).reshape((DEVICES * HOT_LOOK, 1))
    hot_row = touch_ends(ranked_ids(arg_keys[3], (DEVICES, HOT_LOOK), HOT_DEV, 2), jax.random.fold_in(arg_keys[3], 3), 0, HOT_DEV - 1).astype(jnp.int32)
    hot_bag = jax.vmap(lambda own: jnp.searchsorted(jnp.cumsum(ragged_sizes(own, BAGS_DEV, HOT_LOOK, 3 * HOT_LOOK // BAGS_DEV, 2)), jnp.arange(HOT_LOOK), side="right"))(jax.random.split(arg_keys[4], DEVICES)).reshape((DEVICES, HOT_LOOK)).astype(jnp.int32)
    cold_owner_keys = jax.random.split(jax.random.fold_in(arg_keys[5], 1), (DEVICES * COLD_LOOK) // COLD_LOOK)
    cold_owner_turns = jax.random.permutation(jax.random.fold_in(arg_keys[5], 3), (DEVICES * COLD_LOOK) // COLD_LOOK)
    cold_owner = jax.vmap(lambda own, number: deal_out(jax.random.fold_in(arg_keys[5], 2), own, number, COLD_LOOK, N_TT, 1, CAP_COLD, 2))(cold_owner_keys, cold_owner_turns).reshape((DEVICES * COLD_LOOK, 1))
    first_index = touch_ends(jax.random.randint(arg_keys[6], (DEVICES, COLD_LOOK), 0, SLICE_DEV), jax.random.fold_in(arg_keys[6], 1), 0, SLICE_DEV - 1).astype(jnp.int32)
    mid_index = touch_ends(ranked_ids(arg_keys[7], (DEVICES, COLD_LOOK), MID_SLICES, 1), jax.random.fold_in(arg_keys[7], 3), 0, MID_SLICES - 1).astype(jnp.int32)
    last_index = touch_ends(jax.random.randint(arg_keys[8], (DEVICES, COLD_LOOK), 0, LAST_SLICES), jax.random.fold_in(arg_keys[8], 1), 0, LAST_SLICES - 1).astype(jnp.int32)
    cold_bag = jax.vmap(lambda own: jnp.searchsorted(jnp.cumsum(ragged_sizes(own, BAGS_DEV, COLD_LOOK, 3 * COLD_LOOK // BAGS_DEV, 2)), jnp.arange(COLD_LOOK), side="right"))(jax.random.split(arg_keys[9], DEVICES)).reshape((DEVICES, COLD_LOOK)).astype(jnp.int32)
    core_first = scatter_about(arg_keys[10], (N_TT * SLICE_DEV, E1 * RANK), RANK ** -0.5, 1.0, ((0, 16),), jnp.float32)
    core_mid = scatter_about(arg_keys[11], (MID_SLICES, RANK * E2 * RANK), RANK ** -0.5, 1.0)
    core_last = scatter_about(arg_keys[12], (LAST_SLICES, RANK * E3), 1.0, 6.0)
    bag_grads = scatter_about(arg_keys[13], (DEVICES * BAGS_DEV, E), 1.0, 6.0, ((0, 512),))
    return dict(hot_table=hot_table, hot_accum=hot_accum, hot_owner=hot_owner, hot_row=hot_row, hot_bag=hot_bag, cold_owner=cold_owner, first_index=first_index, mid_index=mid_index, last_index=last_index, cold_bag=cold_bag, core_first=core_first, core_mid=core_mid, core_last=core_last, bag_grads=bag_grads)


def rounded(values):
    return lax.optimization_barrier(values.astype(jnp.bfloat16)).astype(jnp.float32)

def reference(hot_table, hot_accum, hot_owner, hot_row, hot_bag, cold_owner, first_index, mid_index, last_index, cold_bag, core_first, core_mid, core_last, bag_grads):
    devices_all = hot_bag.shape[0]
    bag_count = BAGS_DEV
    feature_width = E1 * E2 * E3
    tail_width = E2 * E3
    hot_keys = hot_owner[:, 0].reshape(devices_all, -1) * HOT_DEV + hot_row
    fetched = rounded(hot_table[hot_keys.reshape(-1)])
    device_ids = jnp.arange(devices_all, dtype=jnp.int32)[:, None]
    hot_global = (device_ids * bag_count + hot_bag).reshape(-1).astype(jnp.int32)
    pooled_hot = jax.ops.segment_sum(fetched, hot_global, devices_all * bag_count)
    hot_cot = bag_grads[hot_global].astype(jnp.float32)
    row_grad = jax.ops.segment_sum(hot_cot, hot_keys.reshape(-1), N_HOT * HOT_DEV)
    new_accum = hot_accum + lax.optimization_barrier(jnp.mean(row_grad * row_grad, axis=1))
    new_table = hot_table - 0.1 * row_grad / (jnp.sqrt(new_accum)[:, None] + 1e-08)
    first_global = cold_owner[:, 0].reshape(devices_all, -1) * SLICE_DEV + first_index
    grads_by_device = bag_grads.reshape(devices_all, bag_count, feature_width)

    def one_device(inputs):
        first_rows, middle, lasts, bags, grads = inputs
        mid_cores = core_mid[middle].astype(jnp.float32).reshape(-1, RANK, E2, RANK)
        last_cores = core_last[lasts].astype(jnp.float32).reshape(-1, RANK, E3)
        maps = rounded(jnp.einsum('nawb,nbe->nawe', mid_cores, last_cores).reshape(-1, RANK, tail_width))
        slices = rounded(core_first[first_rows]).reshape(-1, E1, RANK)
        cold_rows = rounded(jnp.einsum('kea,kaj->kej', slices, maps).reshape(-1, feature_width))
        pooled_cold = jax.ops.segment_sum(cold_rows, bags, bag_count)
        cotangent = grads[bags].astype(jnp.float32).reshape(-1, E1, tail_width)
        terms = jnp.einsum('kej,kaj->kea', cotangent, maps).reshape(-1, E1 * RANK)
        return (pooled_cold, terms)
    pooled_cold, terms = lax.map(one_device, (first_global, mid_index, last_index, cold_bag, grads_by_device))
    core_grad = jax.ops.segment_sum(terms.reshape(-1, E1 * RANK), first_global.reshape(-1), N_TT * SLICE_DEV)
    new_first = core_first - 0.01 * core_grad
    pooled = pooled_hot + pooled_cold.reshape(devices_all * bag_count, feature_width)
    return (pooled, new_table, new_accum, new_first)
```

```python
import functools

import jax
import jax.numpy as jnp
from jax import lax
from jax.experimental import pallas as pl
from jax.experimental.pallas import tpu as pltpu
from jax.sharding import PartitionSpec as P

MESH = pl.DeviceIdType.MESH
F32 = jnp.float32
BF16 = jnp.bfloat16

HOTS = 32
TTS = 16
CHIPS = 16
E1, E2, E3, RANK = 8, 8, 4, 32
CAP = 16
HL = 256
CL = 512
BAGS = 64
E = 256
ROWS = 256
SL = 128
MIDS = 64


def nn(a, b):
    return jnp.dot(a, b, preferred_element_type=F32)


def tn(a, b):
    return lax.dot_general(a, b, (((0,), (0,)), ((), ())), preferred_element_type=F32)


def nt(a, b):
    return lax.dot_general(a, b, (((1,), (1,)), ((), ())), preferred_element_type=F32)


def iota(shape, dim):
    return lax.broadcasted_iota(jnp.int32, shape, dim)


def send(src, dst, ssem, rsem, hot, tt):
    pltpu.make_async_remote_copy(
        src_ref=src,
        dst_ref=dst,
        send_sem=ssem,
        recv_sem=rsem,
        device_id=(hot, tt),
        device_id_type=MESH,
    ).start()


def wait(ref, sem):
    pltpu.make_async_copy(ref, ref, sem).wait()


def kernel(
    ht, ha, ho, hr, hb, co, fi, mi, li, cb, cf, mid, last, bg,
    pooled, ntab, nacc, nfirst,
    ids_s, ids_r, hs, hrv, rs, rr, zs, zr, gs, gr,
    G, T, LHS, RHS, M2, OHS, LT, cotT, slT, termsT, rowsT, SBs, RTs, pown, dsn, dr, qs, qr, czs, czr, fs, fr,
    ssem, rsem, c1z_sem, c2z_sem, fr_sem,
):
    h = lax.axis_index("hot")
    t = lax.axis_index("tt")
    c = h // 2
    k = lax.rem(h, 2)
    rg = c // 2
    ch = lax.rem(c, 2)
    tp_me = t // 2
    mine = lax.rem(t, 2) == k

    def rows16(r):
        return pl.ds(pl.multiple_of(r * 16, 16), 16)

    def each(n, me, f):
        def step(d, _):
            f(lax.rem(me + d, n))
            return 0

        lax.fori_loop(1, n, step, 0)

    barrier = pltpu.get_barrier_semaphore()
    each(HOTS, h, lambda p: pl.semaphore_signal(barrier, inc=1, device_id=(p, t), device_id_type=MESH))
    each(TTS, t, lambda p: pl.semaphore_signal(barrier, inc=1, device_id=(h, p), device_id_type=MESH))

    ho_col = ho[...]
    oh_owner = (ho_col == iota((HL, HOTS), 1)).astype(F32)
    tri = (iota((HL, HL), 0) > iota((HL, HL), 1)).astype(BF16)
    eye = iota((HL, HL), 0) == iota((HL, HL), 1)
    before = nn(tri, oh_owner.astype(BF16))
    slot = jnp.sum(before * oh_owner, axis=1, keepdims=True).astype(jnp.int32)
    slot_pick = (ho_col * CAP + slot == iota((HL, HOTS * CAP), 1)).astype(BF16)
    hot_pick = (iota((BAGS, HL), 0) == hb[...]).astype(BF16)
    SBs[...] = nn(hot_pick, slot_pick).astype(BF16)
    hs[...] = tn(SBs[...], bg[...]).astype(BF16).reshape(HOTS, CAP, E)
    row_col = jnp.sum(jnp.where(eye, hr[...].astype(F32), 0.0), axis=1, keepdims=True)
    row_at = jnp.where(slot == iota((HL, 128), 1), row_col + 1.0, 0.0).astype(BF16)
    ids_s[...] = (tn(oh_owner.astype(BF16), row_at) - 1.0).reshape(HOTS, 1, 128)

    @pl.when(mine)
    def _():
        left = cf[rows16(rg), 0:128]
        right = cf[rows16(rg), 128:256]
        G[k, ch, tp_me, rows16(rg), :] = jnp.where(ch == 0, left, right).astype(BF16)

    pl.semaphore_wait(barrier, HOTS - 1 + TTS - 1)

    each(HOTS, h, lambda p: send(ids_s.at[p], ids_r.at[h], ssem.at[0], rsem.at[0], p, t))

    @pl.when(mine)
    def _():
        piece = G.at[k, ch, tp_me, rows16(rg), :]
        each(TTS, t, lambda p: send(piece, piece, ssem.at[1], c1z_sem.at[tp_me], h, p))

    each(HOTS, h, lambda p: send(hs.at[p], hrv.at[h], ssem.at[2], rsem.at[2], p, t))
    ids_r[h] = ids_s[h]
    hrv[h] = hs[h]

    eye_c = iota((CL, CL), 0) == iota((CL, CL), 1)
    owner = jnp.sum(jnp.where(eye_c, co[...].astype(F32), 0.0), axis=0, keepdims=True).astype(jnp.int32)
    key = (owner & 1) * 1024 + (owner >> 1) * SL + fi[...]
    for n in range(4):
        OHS[n * 512 : (n + 1) * 512, :] = (iota((512, CL), 0) + n * 512 == key).astype(BF16)
    cold_pick = (iota((BAGS, CL), 0) == cb[...]).astype(BF16)
    cot = tn(bg[...], cold_pick)
    for n in range(4):
        rowsT[n] = cot[:, n * 128 : (n + 1) * 128]
        for e in range(E3):
            cotT[n, e] = rowsT[n, pl.ds(e, 64, stride=E3), :]
    last_pick = (iota((MIDS, CL), 0) == li[...]).astype(BF16)
    picked = tn(last[...], last_pick)
    for n in range(4):
        M2[n, 0:128, :] = picked[:, n * 128 : (n + 1) * 128]
        for e in range(E3):
            LT[e, :, n * 128 : (n + 1) * 128] = M2[n, pl.ds(e, RANK, stride=E3), :]

    def turn(j, _):
        blk = mid[:, pl.ds(pl.multiple_of(j * 128, 128), 128)].astype(F32).T
        parts = blk.reshape(4, 2, 16, MIDS)
        wide = jnp.concatenate([parts[:, 0], parts[:, 1]], axis=-1).reshape(64, 128)
        T[pl.ds(pl.multiple_of(j * 64, 64), 64), :] = wide
        return 0

    lax.fori_loop(0, 64, turn, 0)
    for n in range(16):
        LHS[:, n * 128 : (n + 1) * 128] = T[pl.ds(n, 256, stride=16), :].astype(BF16)

    wait(ids_r.at[pl.ds(0, HOTS - 1)], rsem.at[0])
    asked = jnp.broadcast_to(ids_r[...], (HOTS, CAP, 128)).reshape(HOTS * CAP, 128)
    at_slot = iota((HOTS * CAP, 128), 1) == lax.rem(iota((HOTS * CAP, 128), 0), CAP)
    asked = jnp.sum(jnp.where(at_slot, asked, 0.0), axis=1, keepdims=True).astype(jnp.int32)
    RTs[...] = (asked == iota((HOTS * CAP, ROWS), 1)).astype(BF16)
    rs[...] = nn(RTs[...], ht[...].astype(BF16)).astype(BF16).reshape(HOTS, CAP, E)
    each(HOTS, h, lambda p: send(rs.at[p], rr.at[h], ssem.at[3], rsem.at[3], p, t))
    rr[h] = rs[h]

    wait(hrv.at[pl.ds(0, HOTS - 1)], rsem.at[2])
    zs[...] = tn(RTs[...], hrv[...].reshape(HOTS * CAP, E)).astype(BF16).reshape(TTS, CAP, E)
    each(TTS, t, lambda p: send(zs.at[p], zr.at[t], ssem.at[4], rsem.at[4], h, p))
    zr[t] = zs[t]

    def from_plane(tp, _):
        @pl.when(tp * 2 + k != t)
        def _():
            wait(G.at[k, ch, 0, rows16(rg), :], c1z_sem.at[tp])

        return 0

    lax.fori_loop(0, 8, from_plane, 0)
    piece8 = G.at[k, ch, :, rows16(rg), :]
    each(CHIPS, c, lambda p: send(piece8, piece8, ssem.at[5], rsem.at[5], p * 2 + k, t))

    def one_e(e, _):
        is_mid = iota((MIDS, CL), 0) == mi[...]
        for n in range(32):
            b = (n % 2) * 16 + n // 2
            row = LT[e, b : b + 1, :]
            RHS[n * MIDS : (n + 1) * MIDS, :] = jnp.where(is_mid, row, 0.0).astype(BF16)
        made = nn(LHS[...], RHS[...])
        made = made.astype(BF16).astype(F32)
        for n in range(4):
            M2[n, pl.ds(pl.multiple_of(e * 256, 256), 256), :] = made[:, n * 128 : (n + 1) * 128]
        return 0

    lax.fori_loop(0, E3, one_e, 0)

    wait(zr.at[pl.ds(0, TTS - 1)], rsem.at[4])
    gs[...] = jnp.sum(zr[...].astype(F32), axis=0).astype(BF16)
    each(TTS, t, lambda p: send(gs, gr.at[t], ssem.at[6], rsem.at[6], h, p))
    gr[t] = gs[...]

    wait(qr.at[pl.ds(0, CHIPS - 1)], rsem.at[5])
    send(G.at[k], G.at[k], ssem.at[7], rsem.at[7], c * 2 + 1 - k, t)

    def back_lanes(kt, _):
        def back_e(e, acc):
            acc = list(acc)
            for w in range(E2):
                tiles = [M2[kt, pl.ds(e * 256 + ab * 64 + w, 8, stride=8), :] for ab in range(4)]
                for e1 in range(E1):
                    cot = cotT[kt, e, e1 * 8 + w : e1 * 8 + w + 1, :]
                    for ab in range(4):
                        acc[e1 * 4 + ab] = acc[e1 * 4 + ab] + cot * tiles[ab]
            return tuple(acc)

        acc = lax.fori_loop(0, E3, back_e, tuple(jnp.zeros((8, 128), F32) for _ in range(32)))
        for i in range(32):
            termsT[kt, i * 8 : (i + 1) * 8, :] = acc[i]
        return 0

    lax.fori_loop(0, 4, back_lanes, 0)
    terms = jnp.concatenate([termsT[n] for n in range(4)], axis=1).astype(BF16)

    def half(which):
        return OHS[pl.ds(pl.multiple_of(which * 1024, 1024), 1024), :]

    other = nt(half(1 - k), terms).astype(BF16)
    dsn[0] = other[:, :128].reshape(8, SL, 128)
    dsn[1] = other[:, 128:].reshape(8, SL, 128)
    send(dsn, dr, ssem.at[8], rsem.at[8], c * 2 + 1 - k, t)
    pown[...] = nt(half(k), terms)

    wait(dr, rsem.at[8])
    for i in range(2):
        mine_f = pown[:, i * 128 : (i + 1) * 128].reshape(8, SL, 128)
        qs[i] = (mine_f + dr[i].astype(F32)).astype(BF16)

    def to_chip(p):
        src = qs.at[lax.rem(p, 2), :, rows16(p // 2), :]
        send(src, qr.at[c], ssem.at[9], rsem.at[9], p * 2 + k, t)

    each(CHIPS, c, to_chip)
    qr[c] = qs[ch, :, rows16(rg), :]

    wait(G.at[0], rsem.at[7])
    for i in range(2):
        got = tn(G[0, i].reshape(1024, 128), OHS[0:1024, :]) + tn(G[1, i].reshape(1024, 128), OHS[1024:2048, :])
        for j in range(16):
            for n in range(4):
                at = (i * 4 + j // 4) * 8
                slT[n, j % 4, at : at + 8, :] = got[j * 8 : (j + 1) * 8, n * 128 : (n + 1) * 128]

    def fore_lanes(kt, _):
        def fore_a(a8, acc):
            acc = list(acc)
            for ai in range(8):
                a = a8 * 8 + ai
                tiles = [M2[kt, pl.ds(pl.multiple_of(e * 256 + a * 8, 8), 8), :] for e in range(E3)]
                for e1 in range(E1):
                    row = slT[kt, a8, e1 * 8 + ai : e1 * 8 + ai + 1, :]
                    for e in range(E3):
                        acc[e1 * 4 + e] = acc[e1 * 4 + e] + row * tiles[e]
            return tuple(acc)

        acc = lax.fori_loop(0, 4, fore_a, tuple(jnp.zeros((8, 128), F32) for _ in range(32)))
        for e1 in range(E1):
            for e in range(E3):
                rowsT[kt, pl.ds(e1 * 32 + e, 8, stride=E3), :] = acc[e1 * 4 + e]
        return 0

    lax.fori_loop(0, 4, fore_lanes, 0)
    cold_pick = (iota((BAGS, CL), 0) == cb[...]).astype(BF16)
    rows_bf = jnp.concatenate([rowsT[n] for n in range(4)], axis=1).astype(BF16)
    wait(rr.at[pl.ds(0, HOTS - 1)], rsem.at[3])
    pooled[...] = nt(cold_pick, rows_bf) + nn(SBs[...], rr[...].reshape(HOTS * CAP, E))

    wait(qr.at[pl.ds(0, CHIPS - 1)], rsem.at[9])
    total = qr[0].astype(F32)
    for i in range(1, CHIPS):
        total = total + qr[i].astype(F32)
    czs[...] = total.astype(BF16)

    def to_owner(tp, _):
        @pl.when(tp * 2 + k != t)
        def _():
            send(czs.at[tp], czr.at[t], ssem.at[10], c2z_sem.at[t], h, tp * 2 + k)

        return 0

    lax.fori_loop(0, 8, to_owner, 0)

    wait(gr.at[pl.ds(0, TTS - 1)], rsem.at[6])
    grad = gr[...].reshape(ROWS, E).astype(F32)
    accum = jnp.sum(jnp.where(eye, ha[...], 0.0), axis=1, keepdims=True)
    accum = accum + jnp.sum(grad * grad, axis=1, keepdims=True) * (1.0 / E)
    ntab[...] = ht[...] - 0.1 * grad / (jnp.sqrt(accum) + 1e-08)
    nacc[...] = jnp.sum(jnp.where(eye, accum, 0.0), axis=0, keepdims=True)

    @pl.when(mine)
    def _():
        czr[t] = czs[tp_me]

        def from_tt(p, _):
            @pl.when(p != t)
            def _():
                wait(czr.at[0], c2z_sem.at[p])

            return 0

        lax.fori_loop(0, TTS, from_tt, 0)
        fs[...] = jnp.sum(czr[...].astype(F32), axis=0)
        fr[c] = fs[...]
        each(HOTS, h, lambda p: send(fs, fr.at[c], ssem.at[11], fr_sem.at[c], p, t))

    def from_chip(p, _):
        @pl.when(p * 2 + lax.rem(t, 2) != h)
        def _():
            wait(fr.at[0], fr_sem.at[p])

        return 0

    lax.fori_loop(0, CHIPS, from_chip, 0)
    for p in range(CHIPS):
        at = (slice((p // 2) * 16, (p // 2) * 16 + 16), slice((p % 2) * 128, (p % 2) * 128 + 128))
        nfirst[at] = cf[at] - 0.01 * fr[p]

    wait(ids_r.at[pl.ds(0, HOTS - 1)], ssem.at[0])
    wait(hrv.at[pl.ds(0, HOTS - 1)], ssem.at[2])
    wait(rr.at[pl.ds(0, HOTS - 1)], ssem.at[3])
    wait(zr.at[pl.ds(0, TTS - 1)], ssem.at[4])
    wait(qr.at[pl.ds(0, CHIPS - 1)], ssem.at[5])
    wait(gr.at[pl.ds(0, TTS - 1)], ssem.at[6])
    wait(G.at[0], ssem.at[7])
    wait(dsn, ssem.at[8])
    wait(qr.at[pl.ds(0, CHIPS - 1)], ssem.at[9])

    @pl.when(mine)
    def _():
        wait(czr.at[pl.ds(0, TTS - 1)], ssem.at[1])
        wait(czr.at[pl.ds(0, 7)], ssem.at[10])
        wait(fr.at[pl.ds(0, HOTS - 1)], ssem.at[11])

    @pl.when(jnp.logical_not(mine))
    def _():
        wait(czr.at[pl.ds(0, 8)], ssem.at[10])


def local(
    hot_table, hot_accum, hot_owner, hot_row, hot_bag, cold_owner, first_index, mid_index, last_index, cold_bag,
    core_first, core_mid, core_last, bag_grads,
):
    vm = pl.BlockSpec(memory_space=pltpu.VMEM)
    v = pltpu.VMEM
    outs = (
        jax.ShapeDtypeStruct((BAGS, E), F32),
        jax.ShapeDtypeStruct((ROWS, E), F32),
        jax.ShapeDtypeStruct((1, ROWS), F32),
        jax.ShapeDtypeStruct((SL, E), F32),
    )
    scratch = [
        v((HOTS, 1, 128), F32),
        v((HOTS, 1, 128), F32),
        v((HOTS, CAP, E), BF16),
        v((HOTS, CAP, E), BF16),
        v((HOTS, CAP, E), BF16),
        v((HOTS, CAP, E), BF16),
        v((TTS, CAP, E), BF16),
        v((TTS, CAP, E), BF16),
        v((CAP, E), BF16),
        v((TTS, CAP, E), BF16),
        v((2, 2, 8, SL, 128), BF16),
        v((4096, 128), F32),
        v((256, 2048), BF16),
        v((2048, CL), BF16),
        v((4, 1024, 128), F32),
        v((2048, CL), BF16),
        v((E3, RANK, CL), F32),
        v((4, E3, 64, 128), F32),
        v((4, 4, 64, 128), F32),
        v((4, E, 128), F32),
        v((4, E, 128), F32),
        v((BAGS, HOTS * CAP), BF16),
        v((HOTS * CAP, ROWS), BF16),
        v((1024, E), F32),
        v((2, 8, SL, 128), BF16),
        v((2, 8, SL, 128), BF16),
        v((2, 8, SL, 128), BF16),
        v((CHIPS, 8, 16, 128), BF16),
        v((8, 16, 128), BF16),
        v((TTS, 16, 128), BF16),
        v((16, 128), F32),
        v((HOTS, 16, 128), F32),
        pltpu.SemaphoreType.DMA((12,)),
        pltpu.SemaphoreType.DMA((12,)),
        pltpu.SemaphoreType.DMA((8,)),
        pltpu.SemaphoreType.DMA((TTS,)),
        pltpu.SemaphoreType.DMA((CHIPS,)),
    ]
    pooled, new_table, new_accum, new_first = pl.pallas_call(
        kernel,
        out_shape=outs,
        in_specs=[vm] * 14,
        out_specs=(vm,) * 4,
        scratch_shapes=scratch,
        compiler_params=pltpu.CompilerParams(collective_id=0, has_side_effects=True),
    )(
        hot_table, hot_accum.reshape(1, ROWS), hot_owner, hot_row, hot_bag, cold_owner, first_index, mid_index,
        last_index, cold_bag, core_first, core_mid, core_last, bag_grads,
    )
    return pooled, new_table, new_accum.reshape(ROWS), new_first


def solution(mesh):
    both = P(("hot", "tt"), None)
    placed = (P("hot", None), P("hot"), *((both,) * 8), P("tt", None), P(), P(), both)
    return jax.shard_map(
        local,
        mesh=mesh,
        in_specs=placed,
        out_specs=(both, P("hot", None), P("hot"), P("tt", None)),
        check_vma=False,
    )
```

```python
import functools

import jax
import jax.numpy as jnp
from jax import lax
from jax.experimental import pallas as pl
from jax.experimental.pallas import tpu as pltpu
from jax.sharding import PartitionSpec as P

MESH = pl.DeviceIdType.MESH
F32 = jnp.float32
BF16 = jnp.bfloat16

HOTS = 32
TTS = 16
CHIPS = 16
E1, E2, E3, RANK = 8, 8, 4, 32
CAP = 16
HL = 256
CL = 512
BAGS = 64
E = 256
ROWS = 256
SL = 128
MIDS = 64
LIMIT = 36 * 1024 * 1024


def nn(a, b):
    return jnp.dot(a, b, preferred_element_type=F32)


def tn(a, b):
    return lax.dot_general(a, b, (((0,), (0,)), ((), ())), preferred_element_type=F32)


def nt(a, b):
    return lax.dot_general(a, b, (((1,), (1,)), ((), ())), preferred_element_type=F32)


def iota(shape, dim):
    return lax.broadcasted_iota(jnp.int32, shape, dim)


def send(src, dst, ssem, rsem, hot, tt):
    pltpu.make_async_remote_copy(
        src_ref=src,
        dst_ref=dst,
        send_sem=ssem,
        recv_sem=rsem,
        device_id=(hot, tt),
        device_id_type=MESH,
    ).start()


def wait(ref, sem):
    pltpu.make_async_copy(ref, ref, sem).wait()


def kernel(
    ho_h, hr_h, hb_h, bg_h, co_h, fi_h, cb_h, mi_h, li_h, last_h, cf_h, mid_h, ht_h, ha_h,
    pooled, ntab, nacc, nfirst,
    ho, hr, hb, bg, co, fi, cb, mi, li, last, cf, mid, ht, ha,
    ids_s, ids_r, hs, hrv, rs, rr, zs, zr, gs, gr,
    G, T, LHS, RHS, M2, OHS, LT, cotT, slT, termsT, rowsT, SBs, RTs, pown, dsn, dr, qs, qr, czs, czr, fs, fr,
    isem, ssem, rsem, c1z_sem, c2z_sem, fr_sem,
):
    ins = (ho_h, hr_h, hb_h, bg_h, co_h, fi_h, cb_h, mi_h, li_h, last_h, cf_h, mid_h, ht_h, ha_h)
    held = (ho, hr, hb, bg, co, fi, cb, mi, li, last, cf, mid, ht, ha)

    def fetch(i):
        return pltpu.make_async_copy(ins[i], held[i], isem.at[i])

    def need(*which):
        for i in which:
            fetch(i).wait()

    for i in range(len(ins)):
        fetch(i).start()

    h = lax.axis_index("hot")
    t = lax.axis_index("tt")
    c = h // 2
    k = lax.rem(h, 2)
    rg = c // 2
    ch = lax.rem(c, 2)
    tp_me = t // 2
    mine = lax.rem(t, 2) == k

    def rows16(r):
        return pl.ds(pl.multiple_of(r * 16, 16), 16)

    def each(n, me, f):
        def step(d, _):
            f(lax.rem(me + d, n))
            return 0

        lax.fori_loop(1, n, step, 0)

    barrier = pltpu.get_barrier_semaphore()
    each(HOTS, h, lambda p: pl.semaphore_signal(barrier, inc=1, device_id=(p, t), device_id_type=MESH))
    each(TTS, t, lambda p: pl.semaphore_signal(barrier, inc=1, device_id=(h, p), device_id_type=MESH))

    need(0, 1, 2, 3)
    eye = iota((HL, HL), 0) == iota((HL, HL), 1)
    ho_col = jnp.sum(jnp.where(eye, ho[...].astype(F32), 0.0), axis=1, keepdims=True).astype(jnp.int32)
    oh_owner = (ho_col == iota((HL, HOTS), 1)).astype(F32)
    tri = (iota((HL, HL), 0) > iota((HL, HL), 1)).astype(BF16)
    before = nn(tri, oh_owner.astype(BF16))
    slot = jnp.sum(before * oh_owner, axis=1, keepdims=True).astype(jnp.int32)
    slot_pick = (ho_col * CAP + slot == iota((HL, HOTS * CAP), 1)).astype(BF16)
    hot_pick = (iota((BAGS, HL), 0) == hb[...]).astype(BF16)
    SBs[...] = nn(hot_pick, slot_pick).astype(BF16)
    hs[...] = tn(SBs[...], bg[...]).astype(BF16).reshape(HOTS, CAP, E)
    row_col = jnp.sum(jnp.where(eye, hr[...].astype(F32), 0.0), axis=1, keepdims=True)
    row_at = jnp.where(slot == iota((HL, 128), 1), row_col + 1.0, 0.0).astype(BF16)
    ids_s[...] = (tn(oh_owner.astype(BF16), row_at) - 1.0).reshape(HOTS, 1, 128)

    need(10)
    @pl.when(mine)
    def _():
        left = cf[rows16(rg), 0:128]
        right = cf[rows16(rg), 128:256]
        G[k, ch, tp_me, rows16(rg), :] = jnp.where(ch == 0, left, right).astype(BF16)

    pl.semaphore_wait(barrier, HOTS - 1 + TTS - 1)

    each(HOTS, h, lambda p: send(ids_s.at[p], ids_r.at[h], ssem.at[0], rsem.at[0], p, t))

    @pl.when(mine)
    def _():
        piece = G.at[k, ch, tp_me, rows16(rg), :]
        each(TTS, t, lambda p: send(piece, piece, ssem.at[1], c1z_sem.at[tp_me], h, p))

    each(HOTS, h, lambda p: send(hs.at[p], hrv.at[h], ssem.at[2], rsem.at[2], p, t))
    ids_r[h] = ids_s[h]
    hrv[h] = hs[h]

    need(4, 5, 6, 7, 8, 9)
    owner = co[...]
    key = (owner & 1) * 1024 + (owner >> 1) * SL + fi[...]
    for n in range(4):
        OHS[n * 512 : (n + 1) * 512, :] = (iota((512, CL), 0) + n * 512 == key).astype(BF16)
    cold_pick = (iota((BAGS, CL), 0) == cb[...]).astype(BF16)
    cot = tn(bg[...], cold_pick)
    for n in range(4):
        rowsT[n] = cot[:, n * 128 : (n + 1) * 128]
        for e in range(E3):
            cotT[n, e] = rowsT[n, pl.ds(e, 64, stride=E3), :]
    last_pick = (iota((MIDS, CL), 0) == li[...]).astype(BF16)
    picked = tn(last[...], last_pick)
    for n in range(4):
        M2[n, 0:128, :] = picked[:, n * 128 : (n + 1) * 128]
        for e in range(E3):
            LT[e, :, n * 128 : (n + 1) * 128] = M2[n, pl.ds(e, RANK, stride=E3), :]

    need(11)
    def turn(j, _):
        blk = mid[:, pl.ds(pl.multiple_of(j * 128, 128), 128)].astype(F32).T
        parts = blk.reshape(4, 2, 16, MIDS)
        wide = jnp.concatenate([parts[:, 0], parts[:, 1]], axis=-1).reshape(64, 128)
        T[pl.ds(pl.multiple_of(j * 64, 64), 64), :] = wide
        return 0

    lax.fori_loop(0, 64, turn, 0)
    for n in range(16):
        LHS[:, n * 128 : (n + 1) * 128] = T[pl.ds(n, 256, stride=16), :].astype(BF16)

    def one_e(e, _):
        is_mid = iota((MIDS, CL), 0) == mi[...]
        for n in range(32):
            b = (n % 2) * 16 + n // 2
            row = LT[e, b : b + 1, :]
            RHS[n * MIDS : (n + 1) * MIDS, :] = jnp.where(is_mid, row, 0.0).astype(BF16)
        made = nn(LHS[...], RHS[...])
        made = made.astype(BF16).astype(F32)
        for n in range(4):
            M2[n, pl.ds(pl.multiple_of(e * 256, 256), 256), :] = made[:, n * 128 : (n + 1) * 128]
        return 0

    lax.fori_loop(0, E3, one_e, 0)

    def back_lanes(kt, _):
        def back_e(e, acc):
            acc = list(acc)
            for w in range(E2):
                tiles = [M2[kt, pl.ds(e * 256 + ab * 64 + w, 8, stride=8), :] for ab in range(4)]
                for e1 in range(E1):
                    cot = cotT[kt, e, e1 * 8 + w : e1 * 8 + w + 1, :]
                    for ab in range(4):
                        acc[e1 * 4 + ab] = acc[e1 * 4 + ab] + cot * tiles[ab]
            return tuple(acc)

        acc = lax.fori_loop(0, E3, back_e, tuple(jnp.zeros((8, 128), F32) for _ in range(32)))
        for i in range(32):
            termsT[kt, i * 8 : (i + 1) * 8, :] = acc[i]
        return 0

    lax.fori_loop(0, 4, back_lanes, 0)
    terms = jnp.concatenate([termsT[n] for n in range(4)], axis=1).astype(BF16)

    def half(which):
        return OHS[pl.ds(pl.multiple_of(which * 1024, 1024), 1024), :]

    other = nt(half(1 - k), terms).astype(BF16)
    dsn[0] = other[:, :128].reshape(8, SL, 128)
    dsn[1] = other[:, 128:].reshape(8, SL, 128)
    send(dsn, dr, ssem.at[8], rsem.at[8], c * 2 + 1 - k, t)
    pown[...] = nt(half(k), terms)

    wait(dr, rsem.at[8])
    for i in range(2):
        mine_f = pown[:, i * 128 : (i + 1) * 128].reshape(8, SL, 128)
        qs[i] = (mine_f + dr[i].astype(F32)).astype(BF16)

    def to_chip(p):
        src = qs.at[lax.rem(p, 2), :, rows16(p // 2), :]
        send(src, qr.at[c], ssem.at[9], rsem.at[9], p * 2 + k, t)

    each(CHIPS, c, to_chip)
    qr[c] = qs[ch, :, rows16(rg), :]

    wait(ids_r.at[pl.ds(0, HOTS - 1)], rsem.at[0])
    asked = jnp.broadcast_to(ids_r[...], (HOTS, CAP, 128)).reshape(HOTS * CAP, 128)
    at_slot = iota((HOTS * CAP, 128), 1) == lax.rem(iota((HOTS * CAP, 128), 0), CAP)
    asked = jnp.sum(jnp.where(at_slot, asked, 0.0), axis=1, keepdims=True).astype(jnp.int32)
    RTs[...] = (asked == iota((HOTS * CAP, ROWS), 1)).astype(BF16)
    wait(hrv.at[pl.ds(0, HOTS - 1)], rsem.at[2])
    zs[...] = tn(RTs[...], hrv[...].reshape(HOTS * CAP, E)).astype(BF16).reshape(TTS, CAP, E)
    each(TTS, t, lambda p: send(zs.at[p], zr.at[t], ssem.at[4], rsem.at[4], h, p))
    zr[t] = zs[t]

    need(12)
    rs[...] = nn(RTs[...], ht[...].astype(BF16)).astype(BF16).reshape(HOTS, CAP, E)
    each(HOTS, h, lambda p: send(rs.at[p], rr.at[h], ssem.at[3], rsem.at[3], p, t))
    rr[h] = rs[h]

    def from_plane(tp, _):
        @pl.when(tp * 2 + k != t)
        def _():
            wait(G.at[k, ch, 0, rows16(rg), :], c1z_sem.at[tp])

        return 0

    lax.fori_loop(0, 8, from_plane, 0)
    piece8 = G.at[k, ch, :, rows16(rg), :]
    each(CHIPS, c, lambda p: send(piece8, piece8, ssem.at[5], rsem.at[5], p * 2 + k, t))

    wait(qr.at[pl.ds(0, CHIPS - 1)], rsem.at[9])
    total = qr[0].astype(F32)
    for i in range(1, CHIPS):
        total = total + qr[i].astype(F32)
    czs[...] = total.astype(BF16)

    def to_owner(tp, _):
        @pl.when(tp * 2 + k != t)
        def _():
            send(czs.at[tp], czr.at[t], ssem.at[10], c2z_sem.at[t], h, tp * 2 + k)

        return 0

    lax.fori_loop(0, 8, to_owner, 0)

    wait(zr.at[pl.ds(0, TTS - 1)], rsem.at[4])
    gs[...] = jnp.sum(zr[...].astype(F32), axis=0).astype(BF16)
    each(TTS, t, lambda p: send(gs, gr.at[t], ssem.at[6], rsem.at[6], h, p))
    gr[t] = gs[...]

    wait(qr.at[pl.ds(0, CHIPS - 1)], rsem.at[5])
    send(G.at[k], G.at[k], ssem.at[7], rsem.at[7], c * 2 + 1 - k, t)

    @pl.when(mine)
    def _():
        czr[t] = czs[tp_me]

        def from_tt(p, _):
            @pl.when(p != t)
            def _():
                wait(czr.at[0], c2z_sem.at[p])

            return 0

        lax.fori_loop(0, TTS, from_tt, 0)
        fs[...] = jnp.sum(czr[...].astype(F32), axis=0)
        fr[c] = fs[...]
        each(HOTS, h, lambda p: send(fs, fr.at[c], ssem.at[11], fr_sem.at[c], p, t))

    wait(G.at[0], rsem.at[7])
    for i in range(2):
        got = tn(G[0, i].reshape(1024, 128), OHS[0:1024, :]) + tn(G[1, i].reshape(1024, 128), OHS[1024:2048, :])
        for j in range(16):
            for n in range(4):
                at = (i * 4 + j // 4) * 8
                slT[n, j % 4, at : at + 8, :] = got[j * 8 : (j + 1) * 8, n * 128 : (n + 1) * 128]

    def fore_lanes(kt, _):
        def fore_a(a8, acc):
            acc = list(acc)
            for ai in range(8):
                a = a8 * 8 + ai
                tiles = [M2[kt, pl.ds(pl.multiple_of(e * 256 + a * 8, 8), 8), :] for e in range(E3)]
                for e1 in range(E1):
                    row = slT[kt, a8, e1 * 8 + ai : e1 * 8 + ai + 1, :]
                    for e in range(E3):
                        acc[e1 * 4 + e] = acc[e1 * 4 + e] + row * tiles[e]
            return tuple(acc)

        acc = lax.fori_loop(0, 4, fore_a, tuple(jnp.zeros((8, 128), F32) for _ in range(32)))
        for e1 in range(E1):
            for e in range(E3):
                rowsT[kt, pl.ds(e1 * 32 + e, 8, stride=E3), :] = acc[e1 * 4 + e]
        return 0

    lax.fori_loop(0, 4, fore_lanes, 0)
    cold_pick = (iota((BAGS, CL), 0) == cb[...]).astype(BF16)
    rows_bf = jnp.concatenate([rowsT[n] for n in range(4)], axis=1).astype(BF16)
    wait(rr.at[pl.ds(0, HOTS - 1)], rsem.at[3])
    pooled[...] = nt(cold_pick, rows_bf) + nn(SBs[...], rr[...].reshape(HOTS * CAP, E))

    need(13)
    wait(gr.at[pl.ds(0, TTS - 1)], rsem.at[6])
    grad = gr[...].reshape(ROWS, E).astype(F32)
    accum = jnp.sum(jnp.where(eye, ha[...], 0.0), axis=1, keepdims=True)
    accum = accum + jnp.sum(grad * grad, axis=1, keepdims=True) * (1.0 / E)
    ntab[...] = ht[...] - 0.1 * grad / (jnp.sqrt(accum) + 1e-08)
    nacc[...] = jnp.sum(jnp.where(eye, accum, 0.0), axis=0, keepdims=True)

    def from_chip(p, _):
        @pl.when(p * 2 + lax.rem(t, 2) != h)
        def _():
            wait(fr.at[0], fr_sem.at[p])

        return 0

    lax.fori_loop(0, CHIPS, from_chip, 0)
    for p in range(CHIPS):
        at = (slice((p // 2) * 16, (p // 2) * 16 + 16), slice((p % 2) * 128, (p % 2) * 128 + 128))
        nfirst[at] = cf[at] - 0.01 * fr[p]

    wait(ids_r.at[pl.ds(0, HOTS - 1)], ssem.at[0])
    wait(hrv.at[pl.ds(0, HOTS - 1)], ssem.at[2])
    wait(rr.at[pl.ds(0, HOTS - 1)], ssem.at[3])
    wait(zr.at[pl.ds(0, TTS - 1)], ssem.at[4])
    wait(qr.at[pl.ds(0, CHIPS - 1)], ssem.at[5])
    wait(gr.at[pl.ds(0, TTS - 1)], ssem.at[6])
    wait(G.at[0], ssem.at[7])
    wait(dsn, ssem.at[8])
    wait(qr.at[pl.ds(0, CHIPS - 1)], ssem.at[9])

    @pl.when(mine)
    def _():
        wait(czr.at[pl.ds(0, TTS - 1)], ssem.at[1])
        wait(czr.at[pl.ds(0, 7)], ssem.at[10])
        wait(fr.at[pl.ds(0, HOTS - 1)], ssem.at[11])

    @pl.when(jnp.logical_not(mine))
    def _():
        wait(czr.at[pl.ds(0, 8)], ssem.at[10])


def put_out(a_v, b_v, c_v, d_v, a_h, b_h, c_h, d_h, sem):
    pairs = ((b_v, b_h), (d_v, d_h), (a_v, a_h), (c_v, c_h))
    for i, (v, h) in enumerate(pairs):
        pltpu.make_async_copy(v, h, sem.at[i]).start()
    for i, (v, h) in enumerate(pairs):
        pltpu.make_async_copy(v, h, sem.at[i]).wait()


def local(
    hot_table, hot_accum, hot_owner, hot_row, hot_bag, cold_owner, first_index, mid_index, last_index, cold_bag,
    core_first, core_mid, core_last, bag_grads,
):
    vm = pl.BlockSpec(memory_space=pltpu.VMEM)
    hbm = pl.BlockSpec(memory_space=pltpu.HBM)
    v = pltpu.VMEM
    outs = (
        jax.ShapeDtypeStruct((BAGS, E), F32),
        jax.ShapeDtypeStruct((ROWS, E), F32),
        jax.ShapeDtypeStruct((1, ROWS), F32),
        jax.ShapeDtypeStruct((SL, E), F32),
    )
    scratch = [
        v((1, HL), jnp.int32),
        v((1, HL), jnp.int32),
        v((1, HL), jnp.int32),
        v((BAGS, E), BF16),
        v((1, CL), jnp.int32),
        v((1, CL), jnp.int32),
        v((1, CL), jnp.int32),
        v((1, CL), jnp.int32),
        v((1, CL), jnp.int32),
        v((MIDS, RANK * E3), BF16),
        v((SL, E), F32),
        v((MIDS, RANK * E2 * RANK), BF16),
        v((ROWS, E), F32),
        v((1, ROWS), F32),
        v((HOTS, 1, 128), F32),
        v((HOTS, 1, 128), F32),
        v((HOTS, CAP, E), BF16),
        v((HOTS, CAP, E), BF16),
        v((HOTS, CAP, E), BF16),
        v((HOTS, CAP, E), BF16),
        v((TTS, CAP, E), BF16),
        v((TTS, CAP, E), BF16),
        v((CAP, E), BF16),
        v((TTS, CAP, E), BF16),
        v((2, 2, 8, SL, 128), BF16),
        v((4096, 128), F32),
        v((256, 2048), BF16),
        v((2048, CL), BF16),
        v((4, 1024, 128), F32),
        v((2048, CL), BF16),
        v((E3, RANK, CL), F32),
        v((4, E3, 64, 128), F32),
        v((4, 4, 64, 128), F32),
        v((4, E, 128), F32),
        v((4, E, 128), F32),
        v((BAGS, HOTS * CAP), BF16),
        v((HOTS * CAP, ROWS), BF16),
        v((1024, E), F32),
        v((2, 8, SL, 128), BF16),
        v((2, 8, SL, 128), BF16),
        v((2, 8, SL, 128), BF16),
        v((CHIPS, 8, 16, 128), BF16),
        v((8, 16, 128), BF16),
        v((TTS, 16, 128), BF16),
        v((16, 128), F32),
        v((HOTS, 16, 128), F32),
        pltpu.SemaphoreType.DMA((14,)),
        pltpu.SemaphoreType.DMA((12,)),
        pltpu.SemaphoreType.DMA((12,)),
        pltpu.SemaphoreType.DMA((8,)),
        pltpu.SemaphoreType.DMA((TTS,)),
        pltpu.SemaphoreType.DMA((CHIPS,)),
    ]
    operands = (
        hot_owner.reshape(1, HL), hot_row, hot_bag, bag_grads, cold_owner.reshape(1, CL), first_index, cold_bag,
        mid_index, last_index, core_last, core_first, core_mid, hot_table, hot_accum.reshape(1, ROWS),
    )
    results = pl.pallas_call(
        kernel,
        out_shape=outs,
        in_specs=[hbm] * 14,
        out_specs=(vm,) * 4,
        scratch_shapes=scratch,
        compiler_params=pltpu.CompilerParams(collective_id=0, has_side_effects=True, vmem_limit_bytes=LIMIT),
    )(*(pltpu.with_memory_space_constraint(a, pltpu.HBM) for a in operands))
    pooled, new_table, new_accum, new_first = pl.pallas_call(
        put_out,
        out_shape=outs,
        in_specs=[vm] * 4,
        out_specs=(hbm,) * 4,
        scratch_shapes=[pltpu.SemaphoreType.DMA((4,))],
        compiler_params=pltpu.CompilerParams(vmem_limit_bytes=4 * 1024 * 1024),
    )(*results)
    return pooled, new_table, new_accum.reshape(ROWS), new_first


def solution(mesh):
    both = P(("hot", "tt"), None)
    placed = (P("hot", None), P("hot"), *((both,) * 8), P("tt", None), P(), P(), both)
    return jax.shard_map(
        local,
        mesh=mesh,
        in_specs=placed,
        out_specs=(both, P("hot", None), P("hot"), P("tt", None)),
        check_vma=False,
    )
```

```python
import functools

import jax
import jax.numpy as jnp
from jax import lax
from jax.experimental import pallas as pl
from jax.experimental.pallas import tpu as pltpu
from jax.sharding import PartitionSpec as P

MESH = pl.DeviceIdType.MESH
F32 = jnp.float32
BF16 = jnp.bfloat16

HOTS = 32
TTS = 16
CHIPS = 16
E1, E2, E3, RANK = 8, 8, 4, 32
CAP = 16
HL = 256
CL = 512
BAGS = 64
E = 256
ROWS = 256
SL = 128
MIDS = 64
LIMIT = 36 * 1024 * 1024


def nn(a, b):
    return jnp.dot(a, b, preferred_element_type=F32)


def tn(a, b):
    return lax.dot_general(a, b, (((0,), (0,)), ((), ())), preferred_element_type=F32)


def nt(a, b):
    return lax.dot_general(a, b, (((1,), (1,)), ((), ())), preferred_element_type=F32)


def iota(shape, dim):
    return lax.broadcasted_iota(jnp.int32, shape, dim)


def send(src, dst, ssem, rsem, hot, tt):
    pltpu.make_async_remote_copy(
        src_ref=src,
        dst_ref=dst,
        send_sem=ssem,
        recv_sem=rsem,
        device_id=(hot, tt),
        device_id_type=MESH,
    ).start()


def wait(ref, sem):
    pltpu.make_async_copy(ref, ref, sem).wait()


def kernel(
    ho_h, hr_h, hb_h, bg_h, co_h, fi_h, cb_h, mi_h, li_h, last_h, cf_h, mid_h, ht_h, ha_h,
    pooled, ntab, nacc, nfirst,
    ho, hr, hb, bg, co, fi, cb, mi, li, last, cf, mid, ht, ha,
    ids_s, ids_r, hs, hrv, rs, rr, zs, zr, gs, gr,
    G, T, LHS, RHS, M2, OHS, LT, cotT, slT, termsT, rowsT, SBs, RTs, pown, dsn, dr, qs, qr, czs, czr, fs, fr,
    isem, ssem, rsem, c1z_sem, c2z_sem, fr_sem,
):
    ins = (ho_h, hr_h, hb_h, bg_h, co_h, fi_h, cb_h, mi_h, li_h, last_h, cf_h, mid_h, ht_h, ha_h)
    held = (ho, hr, hb, bg, co, fi, cb, mi, li, last, cf, mid, ht, ha)

    def fetch(i):
        return pltpu.make_async_copy(ins[i], held[i], isem.at[i])

    def need(*which):
        for i in which:
            fetch(i).wait()

    for i in range(len(ins)):
        fetch(i).start()

    h = lax.axis_index("hot")
    t = lax.axis_index("tt")
    c = h // 2
    k = lax.rem(h, 2)
    rg = c // 2
    ch = lax.rem(c, 2)
    tp_me = t // 2
    mine = lax.rem(t, 2) == k

    def rows16(r):
        return pl.ds(pl.multiple_of(r * 16, 16), 16)

    def far(i):
        return 2 + 3 * i + 3 * (i // 2) + 2 * (i // 3)

    def each_plane(f):
        def step(i, _):
            py = lax.rem(c // 4 + far(i // 8), 4)
            px = lax.rem(c + far(lax.rem(i // 2, 4)), 4)
            f((py * 4 + px) * 2 + lax.rem(k + i + 1, 2))
            return 0

        lax.fori_loop(0, HOTS - 1, step, 0)

    def each_chip(f):
        def step(i, _):
            f(lax.rem(c // 4 + far(i // 4), 4) * 4 + lax.rem(c + far(lax.rem(i, 4)), 4))
            return 0

        lax.fori_loop(0, CHIPS - 1, step, 0)

    def each_tt(f):
        def step(i, _):
            f(lax.rem(t + 8 + (i // 2) * (1 - 2 * lax.rem(i, 2)), TTS))
            return 0

        lax.fori_loop(1, TTS, step, 0)

    barrier = pltpu.get_barrier_semaphore()
    each_tt(lambda p: pl.semaphore_signal(barrier, inc=1, device_id=(h, p), device_id_type=MESH))
    each_plane(lambda p: pl.semaphore_signal(barrier, inc=1, device_id=(p, t), device_id_type=MESH))

    need(0, 1, 2, 3)
    eye = iota((HL, HL), 0) == iota((HL, HL), 1)
    ho_col = jnp.sum(jnp.where(eye, ho[...].astype(F32), 0.0), axis=1, keepdims=True).astype(jnp.int32)
    oh_owner = (ho_col == iota((HL, HOTS), 1)).astype(F32)
    tri = (iota((HL, HL), 0) > iota((HL, HL), 1)).astype(BF16)
    before = nn(tri, oh_owner.astype(BF16))
    slot = jnp.sum(before * oh_owner, axis=1, keepdims=True).astype(jnp.int32)
    slot_pick = (ho_col * CAP + slot == iota((HL, HOTS * CAP), 1)).astype(BF16)
    hot_pick = (iota((BAGS, HL), 0) == hb[...]).astype(BF16)
    SBs[...] = nn(hot_pick, slot_pick).astype(BF16)
    hs[...] = tn(SBs[...], bg[...]).astype(BF16).reshape(HOTS, CAP, E)
    row_col = jnp.sum(jnp.where(eye, hr[...].astype(F32), 0.0), axis=1, keepdims=True)
    row_at = jnp.where(slot == iota((HL, 128), 1), row_col + 1.0, 0.0).astype(BF16)
    ids_s[...] = (tn(oh_owner.astype(BF16), row_at) - 1.0).reshape(HOTS, 1, 128)

    need(4, 5, 6, 7, 8, 9)
    owner = co[...]
    key = (owner & 1) * 1024 + (owner >> 1) * SL + fi[...]
    for n in range(4):
        OHS[n * 512 : (n + 1) * 512, :] = (iota((512, CL), 0) + n * 512 == key).astype(BF16)
    cold_pick = (iota((BAGS, CL), 0) == cb[...]).astype(BF16)
    cot = tn(bg[...], cold_pick)
    for n in range(4):
        rowsT[n] = cot[:, n * 128 : (n + 1) * 128]
        for e in range(E3):
            cotT[n, e] = rowsT[n, pl.ds(e, 64, stride=E3), :]
    last_pick = (iota((MIDS, CL), 0) == li[...]).astype(BF16)
    picked = tn(last[...], last_pick)
    for n in range(4):
        M2[n, 0:128, :] = picked[:, n * 128 : (n + 1) * 128]
        for e in range(E3):
            LT[e, :, n * 128 : (n + 1) * 128] = M2[n, pl.ds(e, RANK, stride=E3), :]

    need(10)
    @pl.when(mine)
    def _():
        left = cf[rows16(rg), 0:128]
        right = cf[rows16(rg), 128:256]
        G[k, ch, tp_me, rows16(rg), :] = jnp.where(ch == 0, left, right).astype(BF16)

    need(11)
    def turn(g, _):
        for u in range(8):
            j = g * 8 + u
            blk = mid[:, pl.ds(pl.multiple_of(j * 128, 128), 128)].astype(F32).T
            parts = blk.reshape(4, 2, 16, MIDS)
            wide = jnp.concatenate([parts[:, 0], parts[:, 1]], axis=-1).reshape(64, 128)
            T[pl.ds(pl.multiple_of(j * 64, 64), 64), :] = wide
        return 0

    lax.fori_loop(0, 8, turn, 0)
    for n in range(16):
        LHS[:, n * 128 : (n + 1) * 128] = T[pl.ds(n, 256, stride=16), :].astype(BF16)

    pl.semaphore_wait(barrier, HOTS - 1 + TTS - 1)

    each_plane(lambda p: send(ids_s.at[p], ids_r.at[h], ssem.at[0], rsem.at[0], p, t))

    @pl.when(mine)
    def _():
        piece = G.at[k, ch, tp_me, rows16(rg), :]
        each_tt(lambda p: send(piece, piece, ssem.at[1], c1z_sem.at[tp_me], h, p))

    each_plane(lambda p: send(hs.at[p], hrv.at[h], ssem.at[2], rsem.at[2], p, t))
    ids_r[h] = ids_s[h]
    hrv[h] = hs[h]

    def one_e(e, _):
        is_mid = iota((MIDS, CL), 0) == mi[...]
        for n in range(32):
            b = (n % 2) * 16 + n // 2
            row = LT[e, b : b + 1, :]
            RHS[n * MIDS : (n + 1) * MIDS, :] = jnp.where(is_mid, row, 0.0).astype(BF16)
        made = nn(LHS[...], RHS[...])
        made = made.astype(BF16).astype(F32)
        for n in range(4):
            M2[n, pl.ds(pl.multiple_of(e * 256, 256), 256), :] = made[:, n * 128 : (n + 1) * 128]
        return 0

    lax.fori_loop(0, E3, one_e, 0)

    def back_lanes(kt, _):
        def back_e(e, acc):
            acc = list(acc)
            for w in range(E2):
                tiles = [M2[kt, pl.ds(e * 256 + ab * 64 + w, 8, stride=8), :] for ab in range(4)]
                for e1 in range(E1):
                    cot = cotT[kt, e, e1 * 8 + w : e1 * 8 + w + 1, :]
                    for ab in range(4):
                        acc[e1 * 4 + ab] = acc[e1 * 4 + ab] + cot * tiles[ab]
            return tuple(acc)

        acc = lax.fori_loop(0, E3, back_e, tuple(jnp.zeros((8, 128), F32) for _ in range(32)))
        for i in range(32):
            termsT[kt, i * 8 : (i + 1) * 8, :] = acc[i]
        return 0

    lax.fori_loop(0, 4, back_lanes, 0)
    terms = jnp.concatenate([termsT[n] for n in range(4)], axis=1).astype(BF16)

    def half(which):
        return OHS[pl.ds(pl.multiple_of(which * 1024, 1024), 1024), :]

    for i in range(2):
        dsn[i] = nt(half(1 - k), terms[i * 128 : (i + 1) * 128]).astype(BF16).reshape(8, SL, 128)
        send(dsn.at[i], dr.at[i], ssem.at[8], rsem.at[8 + 6 * i], c * 2 + 1 - k, t)
    pown[...] = nt(half(k), terms)

    wait(ids_r.at[pl.ds(0, HOTS - 1)], rsem.at[0])
    asked = jnp.broadcast_to(ids_r[...], (HOTS, CAP, 128)).reshape(HOTS * CAP, 128)
    at_slot = iota((HOTS * CAP, 128), 1) == lax.rem(iota((HOTS * CAP, 128), 0), CAP)
    asked = jnp.sum(jnp.where(at_slot, asked, 0.0), axis=1, keepdims=True).astype(jnp.int32)
    RTs[...] = (asked == iota((HOTS * CAP, ROWS), 1)).astype(BF16)
    for i in range(2):
        wait(dr.at[i], rsem.at[8 + 6 * i])
        mine_f = pown[:, i * 128 : (i + 1) * 128].reshape(8, SL, 128)
        qs[i] = (mine_f + dr[i].astype(F32)).astype(BF16)

    def to_chip(p):
        src = qs.at[lax.rem(p, 2), :, rows16(p // 2), :]
        send(src, qr.at[c], ssem.at[9], rsem.at[9], p * 2 + k, t)

    each_chip(to_chip)
    qr[c] = qs[ch, :, rows16(rg), :]

    wait(hrv.at[pl.ds(0, HOTS - 1)], rsem.at[2])
    part = tn(RTs[...], hrv[...].reshape(HOTS * CAP, E)).astype(BF16)
    for i in range(2):
        zs[i] = part[:, i * 128 : (i + 1) * 128].reshape(TTS, CAP, 128)
        each_tt(lambda p: send(zs.at[i, p], zr.at[i, t], ssem.at[4], rsem.at[4 + 8 * i], h, p))
        zr[i, t] = zs[i, t]

    need(12)
    rs[...] = nn(RTs[...], ht[...].astype(BF16)).astype(BF16).reshape(HOTS, CAP, E)
    each_plane(lambda p: send(rs.at[p], rr.at[h], ssem.at[3], rsem.at[3], p, t))
    rr[h] = rs[h]

    def from_plane(tp, _):
        @pl.when(tp * 2 + k != t)
        def _():
            wait(G.at[k, ch, 0, rows16(rg), :], c1z_sem.at[tp])

        return 0

    lax.fori_loop(0, 8, from_plane, 0)
    piece8 = G.at[k, ch, :, rows16(rg), :]
    each_chip(lambda p: send(piece8, piece8, ssem.at[5], rsem.at[5], p * 2 + k, t))

    wait(zr.at[0, pl.ds(0, TTS - 1)], rsem.at[4])
    gs[0] = jnp.sum(zr[0].astype(F32), axis=0).astype(BF16)
    each_tt(lambda p: send(gs.at[0], gr.at[0, t], ssem.at[6], rsem.at[6], h, p))
    gr[0, t] = gs[0]

    wait(qr.at[pl.ds(0, CHIPS - 1)], rsem.at[9])
    total = qr[0].astype(F32)
    for i in range(1, CHIPS):
        total = total + qr[i].astype(F32)
    czs[...] = total.astype(BF16)

    def to_owner(tp, _):
        @pl.when(tp * 2 + k != t)
        def _():
            send(czs.at[tp], czr.at[t], ssem.at[10], c2z_sem.at[t], h, tp * 2 + k)

        return 0

    lax.fori_loop(0, 8, to_owner, 0)

    wait(zr.at[1, pl.ds(0, TTS - 1)], rsem.at[12])
    gs[1] = jnp.sum(zr[1].astype(F32), axis=0).astype(BF16)
    each_tt(lambda p: send(gs.at[1], gr.at[1, t], ssem.at[6], rsem.at[13], h, p))
    gr[1, t] = gs[1]

    wait(qr.at[pl.ds(0, CHIPS - 1)], rsem.at[5])
    send(G.at[k], G.at[k], ssem.at[7], rsem.at[7], c * 2 + 1 - k, t)

    @pl.when(mine)
    def _():
        czr[t] = czs[tp_me]

        def from_tt(p, _):
            @pl.when(p != t)
            def _():
                wait(czr.at[0], c2z_sem.at[p])

            return 0

        lax.fori_loop(0, TTS, from_tt, 0)
        fs[...] = jnp.sum(czr[...].astype(F32), axis=0)
        fr[c] = fs[...]
        each_plane(lambda p: send(fs, fr.at[c], ssem.at[11], fr_sem.at[c], p, t))

    wait(G.at[0], rsem.at[7])
    for i in range(2):
        got = tn(G[0, i].reshape(1024, 128), OHS[0:1024, :]) + tn(G[1, i].reshape(1024, 128), OHS[1024:2048, :])
        for j in range(16):
            for n in range(4):
                at = (i * 4 + j // 4) * 8
                slT[n, j % 4, at : at + 8, :] = got[j * 8 : (j + 1) * 8, n * 128 : (n + 1) * 128]

    def fore_lanes(kt, _):
        def fore_a(a8, acc):
            acc = list(acc)
            for ai in range(8):
                a = a8 * 8 + ai
                tiles = [M2[kt, pl.ds(pl.multiple_of(e * 256 + a * 8, 8), 8), :] for e in range(E3)]
                for e1 in range(E1):
                    row = slT[kt, a8, e1 * 8 + ai : e1 * 8 + ai + 1, :]
                    for e in range(E3):
                        acc[e1 * 4 + e] = acc[e1 * 4 + e] + row * tiles[e]
            return tuple(acc)

        acc = lax.fori_loop(0, 4, fore_a, tuple(jnp.zeros((8, 128), F32) for _ in range(32)))
        for e1 in range(E1):
            for e in range(E3):
                rowsT[kt, pl.ds(e1 * 32 + e, 8, stride=E3), :] = acc[e1 * 4 + e]
        return 0

    lax.fori_loop(0, 4, fore_lanes, 0)
    cold_pick = (iota((BAGS, CL), 0) == cb[...]).astype(BF16)
    rows_bf = jnp.concatenate([rowsT[n] for n in range(4)], axis=1).astype(BF16)
    wait(rr.at[pl.ds(0, HOTS - 1)], rsem.at[3])
    pooled[...] = nt(cold_pick, rows_bf) + nn(SBs[...], rr[...].reshape(HOTS * CAP, E))

    need(13)
    wait(gr.at[0, pl.ds(0, TTS - 1)], rsem.at[6])
    wait(gr.at[1, pl.ds(0, TTS - 1)], rsem.at[13])
    grad = jnp.concatenate([gr[0].reshape(ROWS, 128), gr[1].reshape(ROWS, 128)], axis=1).astype(F32)
    accum = jnp.sum(jnp.where(eye, ha[...], 0.0), axis=1, keepdims=True)
    accum = accum + jnp.sum(grad * grad, axis=1, keepdims=True) * (1.0 / E)
    ntab[...] = ht[...] - 0.1 * grad / (jnp.sqrt(accum) + 1e-08)
    nacc[...] = jnp.sum(jnp.where(eye, accum, 0.0), axis=0, keepdims=True)

    def from_chip(p, _):
        @pl.when(p * 2 + lax.rem(t, 2) != h)
        def _():
            wait(fr.at[0], fr_sem.at[p])

        return 0

    lax.fori_loop(0, CHIPS, from_chip, 0)
    for p in range(CHIPS):
        at = (slice((p // 2) * 16, (p // 2) * 16 + 16), slice((p % 2) * 128, (p % 2) * 128 + 128))
        nfirst[at] = cf[at] - 0.01 * fr[p]

    wait(ids_r.at[pl.ds(0, HOTS - 1)], ssem.at[0])
    wait(hrv.at[pl.ds(0, HOTS - 1)], ssem.at[2])
    wait(rr.at[pl.ds(0, HOTS - 1)], ssem.at[3])
    wait(zr.at[:, pl.ds(0, TTS - 1)], ssem.at[4])
    wait(qr.at[pl.ds(0, CHIPS - 1)], ssem.at[5])
    wait(gr.at[:, pl.ds(0, TTS - 1)], ssem.at[6])
    wait(G.at[0], ssem.at[7])
    wait(dsn, ssem.at[8])
    wait(qr.at[pl.ds(0, CHIPS - 1)], ssem.at[9])

    @pl.when(mine)
    def _():
        wait(czr.at[pl.ds(0, TTS - 1)], ssem.at[1])
        wait(czr.at[pl.ds(0, 7)], ssem.at[10])
        wait(fr.at[pl.ds(0, HOTS - 1)], ssem.at[11])

    @pl.when(jnp.logical_not(mine))
    def _():
        wait(czr.at[pl.ds(0, 8)], ssem.at[10])


def put_out(a_v, b_v, c_v, d_v, a_h, b_h, c_h, d_h, sem):
    pairs = ((b_v, b_h), (d_v, d_h), (a_v, a_h), (c_v, c_h))
    for i, (v, h) in enumerate(pairs):
        pltpu.make_async_copy(v, h, sem.at[i]).start()
    for i, (v, h) in enumerate(pairs):
        pltpu.make_async_copy(v, h, sem.at[i]).wait()


def local(
    hot_table, hot_accum, hot_owner, hot_row, hot_bag, cold_owner, first_index, mid_index, last_index, cold_bag,
    core_first, core_mid, core_last, bag_grads,
):
    vm = pl.BlockSpec(memory_space=pltpu.VMEM)
    hbm = pl.BlockSpec(memory_space=pltpu.HBM)
    v = pltpu.VMEM
    outs = (
        jax.ShapeDtypeStruct((BAGS, E), F32),
        jax.ShapeDtypeStruct((ROWS, E), F32),
        jax.ShapeDtypeStruct((1, ROWS), F32),
        jax.ShapeDtypeStruct((SL, E), F32),
    )
    scratch = [
        v((1, HL), jnp.int32),
        v((1, HL), jnp.int32),
        v((1, HL), jnp.int32),
        v((BAGS, E), BF16),
        v((1, CL), jnp.int32),
        v((1, CL), jnp.int32),
        v((1, CL), jnp.int32),
        v((1, CL), jnp.int32),
        v((1, CL), jnp.int32),
        v((MIDS, RANK * E3), BF16),
        v((SL, E), F32),
        v((MIDS, RANK * E2 * RANK), BF16),
        v((ROWS, E), F32),
        v((1, ROWS), F32),
        v((HOTS, 1, 128), F32),
        v((HOTS, 1, 128), F32),
        v((HOTS, CAP, E), BF16),
        v((HOTS, CAP, E), BF16),
        v((HOTS, CAP, E), BF16),
        v((HOTS, CAP, E), BF16),
        v((2, TTS, CAP, 128), BF16),
        v((2, TTS, CAP, 128), BF16),
        v((2, CAP, 128), BF16),
        v((2, TTS, CAP, 128), BF16),
        v((2, 2, 8, SL, 128), BF16),
        v((4096, 128), F32),
        v((256, 2048), BF16),
        v((2048, CL), BF16),
        v((4, 1024, 128), F32),
        v((2048, CL), BF16),
        v((E3, RANK, CL), F32),
        v((4, E3, 64, 128), F32),
        v((4, 4, 64, 128), F32),
        v((4, E, 128), F32),
        v((4, E, 128), F32),
        v((BAGS, HOTS * CAP), BF16),
        v((HOTS * CAP, ROWS), BF16),
        v((1024, E), F32),
        v((2, 8, SL, 128), BF16),
        v((2, 8, SL, 128), BF16),
        v((2, 8, SL, 128), BF16),
        v((CHIPS, 8, 16, 128), BF16),
        v((8, 16, 128), BF16),
        v((TTS, 16, 128), BF16),
        v((16, 128), F32),
        v((HOTS, 16, 128), F32),
        pltpu.SemaphoreType.DMA((14,)),
        pltpu.SemaphoreType.DMA((16,)),
        pltpu.SemaphoreType.DMA((16,)),
        pltpu.SemaphoreType.DMA((8,)),
        pltpu.SemaphoreType.DMA((TTS,)),
        pltpu.SemaphoreType.DMA((CHIPS,)),
    ]
    operands = (
        hot_owner.reshape(1, HL), hot_row, hot_bag, bag_grads, cold_owner.reshape(1, CL), first_index, cold_bag,
        mid_index, last_index, core_last, core_first, core_mid, hot_table, hot_accum.reshape(1, ROWS),
    )
    results = pl.pallas_call(
        kernel,
        out_shape=outs,
        in_specs=[hbm] * 14,
        out_specs=(vm,) * 4,
        scratch_shapes=scratch,
        compiler_params=pltpu.CompilerParams(collective_id=0, has_side_effects=True, vmem_limit_bytes=LIMIT),
    )(*(pltpu.with_memory_space_constraint(a, pltpu.HBM) for a in operands))
    pooled, new_table, new_accum, new_first = pl.pallas_call(
        put_out,
        out_shape=outs,
        in_specs=[vm] * 4,
        out_specs=(hbm,) * 4,
        scratch_shapes=[pltpu.SemaphoreType.DMA((4,))],
        compiler_params=pltpu.CompilerParams(vmem_limit_bytes=4 * 1024 * 1024),
    )(*results)
    return pooled, new_table, new_accum.reshape(ROWS), new_first


def solution(mesh):
    both = P(("hot", "tt"), None)
    placed = (P("hot", None), P("hot"), *((both,) * 8), P("tt", None), P(), P(), both)
    return jax.shard_map(
        local,
        mesh=mesh,
        in_specs=placed,
        out_specs=(both, P("hot", None), P("hot"), P("tt", None)),
        check_vma=False,
    )
```
